512 devices in a mesh: expert: 32 (over z_lo, x, core), fsdp: 4 (over z_hi), dp: 4 (over y).
Axes of the slice: x: 4, y: 4, z: 16 (z_hi: 4, z_lo: 4; z = z_hi * 4 + z_lo), core: 2. Of those that a mesh axis runs over, the one named last changes fastest.
Arguments:
- tokens: bfloat16 [8192, 3584], P(('expert', 'fsdp', 'dp')), may hold values from -6 to 6
- routes: int32 [8192, 3], P(('expert', 'fsdp', 'dp')), may hold values from 0 to 31, all different within a row; in each aligned block of 16 rows (0 to 15, 16 to 31, ...) at most 2 rows name the same one
- gate_fixed: int32 [8192, 3], P(('expert', 'fsdp', 'dp')), may hold values from 1 to 65535
- gate_weight: bfloat16 [32, 3584, 1024], P('expert', 'fsdp', 'dp'), may hold values from -0.09375 to 0.09375
- up_weight: bfloat16 [32, 3584, 1024], P('expert', 'fsdp', 'dp'), may hold values from -0.09375 to 0.09375
- down_weight: bfloat16 [32, 1024, 3584], P('expert', 'dp', 'fsdp'), may hold values from -0.1875 to 0.1875
- cotangent: bfloat16 [8192, 3584], P(('expert', 'fsdp', 'dp')), may hold values from -24 to 24
Outputs:
- mixed: bfloat16 [8192, 3584], P(('expert', 'fsdp', 'dp'))
- grad_tokens: bfloat16 [8192, 3584], P(('expert', 'fsdp', 'dp'))
- grad_down: float32 [32, 1024, 3584], P('expert', 'dp', 'fsdp')
- grad_gate: float32 [32, 3584, 1024], P('expert', 'fsdp', 'dp')
- grad_up: float32 [32, 3584, 1024], P('expert', 'fsdp', 'dp')
The draws below stay inside these ranges and needn't reach their ends.
Inputs may be any that keep to these rules, and one draw needn't show every extreme that they name: `routes`: each row names 3 different experts; the 16 rows of one device name any one expert at most 2 times, and in every draw some device names some expert exactly 2 times.
All inputs are finite; a program needn't handle non-finite values.
Results may differ from the reference program's by a relative error of at most 0.0064.
Values may be sent and summed in bfloat16 or wider, within the bound.
A program may use at most 64 MiB of HBM per device.

```python
import math
import jax
import jax.numpy as jnp
import numpy as np
from jax import lax

D = 3584
FF = 1024
TOK_DEV = 16
EXPERTS = 32
TOP = 3
CAP = 2
TOKENS = 8192
N_DP = 4


def place_ends(array, key, low, high):
    index_at = [jax.random.randint(jax.random.fold_in(key, axis), (), 0, length) for axis, length in enumerate(array.shape)]
    main_axis = array.shape.index(max(array.shape))
    neighbour = index_at[:main_axis] + [(index_at[main_axis] + 1) % array.shape[main_axis]] + index_at[main_axis + 1:]
    return array.at[tuple(index_at)].set(low).at[tuple(neighbour)].set(high)


def spiked(result, own_key, source, target, blocks, factor):
    def block_of(dim):
        return (jnp.arange(result.shape[dim]) // (result.shape[dim] // blocks)).reshape((-1,) + (1,) * (result.ndim - 1 - dim))

    one_side = jax.random.permutation(own_key, blocks)[block_of(target)]
    far = (block_of(target) + blocks // 2) % blocks
    return jnp.where((block_of(source) == one_side) | (block_of(source) == far), factor * result, result)


def shard_levels(stream_key, extent, pieces, low, largest):
    level, own = 1.0, jax.random.fold_in(stream_key, 6)
    for position, shards_of in pieces:
        draws = jnp.exp(jax.random.uniform(jax.random.fold_in(own, position), (shards_of,), jnp.float32, low / len(pieces), largest / len(pieces)))
        level = level * jnp.repeat(draws, extent[position] // shards_of).reshape([-1 if axis == position else 1 for axis in range(len(extent))])
    return level


def shared_out(key, own, number, rows, count, top, reach, slope):
    order = jax.random.permutation(key, count)
    heavy_load, usual = load_shares(count, rows * top, reach, slope, True), load_shares(count, rows * top, reach, slope, False)
    places = jnp.arange(count)

    def named(sizes, turn):
        used = int((sizes > 0).sum())
        fixed = max(1, used // 4)
        shifted = fixed + (places - fixed + turn * (used - fixed)) % max(1, count - fixed)
        return jnp.zeros((count,), jnp.int32).at[order[jnp.where(places < fixed, places, shifted)]].set(jnp.asarray(sizes, jnp.int32))

    sizes = jnp.where(number % 4 == 0, named(heavy_load, number // 4), named(usual, number - number // 4 - 1))
    mixed = jax.random.permutation(jax.random.fold_in(own, 3), count)
    giver, taker = mixed[0:count // 2 * 2:2], mixed[1:count // 2 * 2:2]
    room = jnp.minimum(sizes[giver] - 1, reach - sizes[taker]) // 2
    room = jnp.where((giver == order[0]) | (taker == order[0]) | (sizes[taker] == 0), 0, jnp.maximum(room, 0))
    shifted = jax.random.randint(jax.random.fold_in(own, 4), (count // 2,), 0, 1 << 20) % (room + 1)
    sizes = sizes.at[giver].add(-shifted).at[taker].add(shifted)
    members = jnp.searchsorted(jnp.cumsum(sizes), jnp.arange(rows * top), side="right").astype(jnp.int32)
    grid = members.reshape(top, rows).T
    grid = grid[jax.random.permutation(jax.random.fold_in(own, 1), rows)]
    turn = jax.random.randint(jax.random.fold_in(own, 2), (rows, 1), 0, top)
    return jnp.take_along_axis(grid, (jnp.arange(top)[None, :] + turn) % top, axis=1)


def load_shares(number_of, total, bound, slope, full):
    portions = [(1 << 20) // math.isqrt(rank ** slope) + 1 for rank in range(1, number_of + 1)]
    largest = bound if full else min(bound, max(-(-total // number_of), total * portions[0] // sum(portions)))
    least = 1 if total - largest >= number_of - 1 else 0
    counts, spare = [largest] + [least] * (number_of - 1), total - largest - least * (number_of - 1)
    while spare > 0:
        free = [i for i in range(1, number_of) if counts[i] < largest] or [i for i in range(1, number_of) if counts[i] < bound]
        whole, left = sum([portions[i] for i in free]), spare
        for i in free:
            addition = min(bound - counts[i], max(1, left * portions[i] // whole), spare)
            counts[i] = counts[i] + addition
            spare = spare - addition
    return np.array(counts)


def normal_values(rng, extent, scale, bound, shards=(), kind=jnp.bfloat16):
    result = jax.random.normal(rng, extent, jnp.float32) * scale
    if len(shards) > 0:
        result = shard_levels(rng, extent, shards, -0.22, 0.18) * result
    return jnp.clip(result, min=-bound, max=bound).astype(kind)


def noise_with(key, extent, scale, reach, pieces, heavy, held_as=jnp.bfloat16):
    result = scale * jax.random.normal(key, extent, jnp.float32)
    if pieces:
        result = result * shard_levels(key, extent, pieces, -0.22, 0.18)
    return jnp.clip(spiked(result, jax.random.fold_in(key, 3), *heavy), -reach, reach).astype(held_as)


def setup_inputs(seed: int = 0) -> dict:
    key_list = jax.random.split(jax.random.key(seed), 8)
    tokens = normal_values(key_list[0], (TOKENS, D), 1.0, 6.0, ((0, 512),))
    routes_keys = jax.random.split(jax.random.fold_in(key_list[1], 1), TOKENS // TOK_DEV)
    routes_turns = jax.random.permutation(jax.random.fold_in(key_list[1], 3), TOKENS // TOK_DEV)
    routes = jax.vmap(lambda own, number: shared_out(jax.random.fold_in(key_list[1], 2), own, number, TOK_DEV, EXPERTS, TOP, CAP, 2))(routes_keys, routes_turns).reshape((TOKENS, TOP))
    gate_fixed = place_ends(jax.random.randint(key_list[2], (TOKENS, TOP), 1, 65536), jax.random.fold_in(key_list[2], 1), 1, 65535).astype(jnp.int32)
    gate_weight = normal_values(key_list[3], (EXPERTS, D, FF), D ** -0.5, 0.09375, ((0, 32), (1, 4), (2, 4)))
    up_weight = normal_values(key_list[4], (EXPERTS, D, FF), D ** -0.5, 0.09375, ((0, 32), (1, 4), (2, 4)))
    down_weight = normal_values(key_list[5], (EXPERTS, FF, D), FF ** -0.5, 0.1875, ((0, 32), (1, 4), (2, 4)))
    cotangent = noise_with(key_list[6], (TOKENS, D), 1.0, 24.0, ((0, 512),), (0, 1, 512, 6.0))
    return dict(tokens=tokens, routes=routes, gate_fixed=gate_fixed, gate_weight=gate_weight, up_weight=up_weight, down_weight=down_weight, cotangent=cotangent)


def reference(tokens, routes, gate_fixed, gate_weight, up_weight, down_weight, cotangent):
    pair_total = TOKENS * TOP
    flat_ids = routes.reshape(pair_total)
    coefficient = (gate_fixed.astype(jnp.float32) / 65536.0).reshape(pair_total)
    ordering = jnp.argsort(flat_ids, stable=True).astype(jnp.int32)
    row_limit = CAP * (TOKENS // TOK_DEV)
    expert_load = jnp.sum((flat_ids[:, None] == jnp.arange(EXPERTS, dtype=jnp.int32)[None, :]).astype(jnp.int32), axis=0)
    first_pair = (jnp.cumsum(expert_load) - expert_load).astype(jnp.int32)
    padded_order = jnp.concatenate([ordering, jnp.zeros((row_limit,), jnp.int32)])
    slice_width = FF // N_DP

    def per_expert(carry, expert):
        out_acc, grad_acc = carry
        picked = lax.dynamic_slice(padded_order, (first_pair[expert],), (row_limit,))
        live_row = jnp.arange(row_limit, dtype=jnp.int32) < expert_load[expert]
        token_of = picked // TOP
        pair_weight = jnp.where(live_row, coefficient[picked], jnp.float32(0.0))
        expert_rows = jnp.where(live_row[:, None], tokens[token_of], jnp.zeros((), jnp.bfloat16))
        gate_mat = gate_weight[expert]
        up_mat = up_weight[expert]
        down_mat = down_weight[expert]
        gate_pre = jnp.dot(expert_rows, gate_mat, preferred_element_type=jnp.float32)
        up_pre = jnp.dot(expert_rows, up_mat, preferred_element_type=jnp.float32)
        sigmoid_gate = jax.nn.sigmoid(gate_pre)
        swish = gate_pre * sigmoid_gate
        hidden = (swish * up_pre).astype(jnp.bfloat16)
        scaled = (pair_weight[:, None] * cotangent[token_of].astype(jnp.float32)).astype(jnp.bfloat16)
        hidden_grad = jnp.dot(scaled, down_mat.T, preferred_element_type=jnp.float32)
        gate_grad = (hidden_grad * up_pre * sigmoid_gate * (1.0 + gate_pre * (1.0 - sigmoid_gate))).astype(jnp.bfloat16)
        up_grad = (hidden_grad * swish).astype(jnp.bfloat16)
        summed = jnp.zeros((row_limit, D), jnp.float32)
        back_sum = jnp.zeros((row_limit, D), jnp.float32)
        for piece in range(N_DP):
            low = piece * slice_width
            high = low + slice_width
            partial_value = jnp.dot(hidden[:, low:high], down_mat[low:high], preferred_element_type=jnp.float32).astype(jnp.bfloat16)
            summed = summed + partial_value.astype(jnp.float32)
            back = jnp.dot(gate_grad[:, low:high], gate_mat[:, low:high].T, preferred_element_type=jnp.float32)
            back = back + jnp.dot(up_grad[:, low:high], up_mat[:, low:high].T, preferred_element_type=jnp.float32)
            back_sum = back_sum + back.astype(jnp.bfloat16).astype(jnp.float32)
        out_acc = out_acc.at[token_of].add(pair_weight[:, None] * summed)
        grad_acc = grad_acc.at[token_of].add(jnp.where(live_row[:, None], back_sum, jnp.float32(0.0)))
        down_grad = jnp.dot(hidden.T, scaled, preferred_element_type=jnp.float32)
        gate_wgrad = jnp.dot(expert_rows.T, gate_grad, preferred_element_type=jnp.float32)
        up_wgrad = jnp.dot(expert_rows.T, up_grad, preferred_element_type=jnp.float32)
        return (out_acc, grad_acc), (down_grad, gate_wgrad, up_wgrad)

    start = (jnp.zeros((TOKENS, D), jnp.float32), jnp.zeros((TOKENS, D), jnp.float32))
    (out_acc, grad_acc), (grad_down, grad_gate, grad_up) = lax.scan(per_expert, start, jnp.arange(EXPERTS, dtype=jnp.int32))
    return out_acc.astype(jnp.bfloat16), grad_acc.astype(jnp.bfloat16), grad_down, grad_gate, grad_up
```

```python
import functools

import jax
import jax.numpy as jnp
from jax import lax
from jax.experimental import pallas as pl
from jax.experimental.pallas import tpu as pltpu
from jax.sharding import PartitionSpec as P

F32 = jnp.float32
BF16 = jnp.bfloat16
CAP = 2


def log2(number):
    assert number & (number - 1) == 0
    return number.bit_length() - 1


def dot(a, b, ca, cb):
    return lax.dot_general(a, b, (((ca,), (cb,)), ((), ())), preferred_element_type=F32)


def kernel(
    sizes,
    tok_ref, cot_ref, routes_ref, fixed_ref, wg_ref, wu_ref, wd_ref,
    mixed_ref, gtok_ref, gdown_ref, ggate_ref, gup_ref,
    info, xb, xs, xe, pf, rss, rsr, agb, hs, hr, own, isb, irb, mp, ks, kr, ls, lr, w_hi, w_lo, w_one,
    sa, ra, sai, rai, sb, rb, sbi, rbi, sd, rd, se, re, sr, rr, sg, rg, sh, rh, si, ri, sk, rk, sl, rl,
):
    n_zl, n_xc, n_f, n_d = sizes
    n_tok, top = routes_ref.shape
    cols = wg_ref.shape[0]
    hid = wg_ref.shape[1]
    n_src = n_zl * n_f
    col_tok = n_src * n_tok
    slots = n_xc * n_src * CAP
    rows = slots
    part = rows // n_f

    e = lax.axis_index("expert")
    f = lax.axis_index("fsdp")
    d = lax.axis_index("dp")
    zl = e // n_xc
    xc = e % n_xc

    def at_f(j):
        return (f + j) % n_f

    def at_z(j):
        return (zl + j) % n_zl

    def at_x(j):
        return (xc + j) % n_xc

    def at_d(j):
        return (d + j) % n_d

    def device(zl_to=zl, xc_to=xc, f_to=f, d_to=d):
        return {"expert": zl_to * n_xc + xc_to, "fsdp": f_to, "dp": d_to}

    def copy(src, dst, send, recv, **to):
        return pltpu.make_async_remote_copy(
            src_ref=src,
            dst_ref=dst,
            send_sem=send,
            recv_sem=recv,
            device_id=device(**to),
            device_id_type=pl.DeviceIdType.MESH,
        )

    barrier = pltpu.get_barrier_semaphore()
    count = 0
    for limit, name, at in ((n_f, "f_to", at_f), (n_zl, "zl_to", at_z), (n_xc, "xc_to", at_x), (n_d, "d_to", at_d)):
        for j in range(1, limit):
            pl.semaphore_signal(
                barrier, inc=1, device_id=device(**{name: at(j)}), device_id_type=pl.DeviceIdType.MESH
            )
            count += 1

    lane = lax.broadcasted_iota(jnp.int32, (n_tok, 128), 1)
    packed = jnp.zeros((n_tok, 128), jnp.int32)
    for k in range(top):
        packed = jnp.where(lane == k, routes_ref[:, k : k + 1], packed)
        packed = jnp.where(lane == top + k, fixed_ref[:, k : k + 1], packed)
    info[zl, f] = packed
    own_cols = pl.ds(pl.multiple_of(f * cols, 128), cols)
    xb[0, zl, f] = tok_ref[:, own_cols]
    xb[1, zl, f] = cot_ref[:, own_cols]

    pl.semaphore_wait(barrier, count)

    def copy_a(a, j):
        there = at_f(j)
        src = (tok_ref, cot_ref)[a]
        columns = pl.ds(pl.multiple_of(there * cols, 128), cols)
        return copy(src.at[:, columns], xb.at[a, zl, f], sa.at[a, j], ra.at[a, j], f_to=there)

    def copy_ai(j):
        return copy(info.at[zl, f], info.at[zl, f], sai.at[j], rai.at[j], f_to=at_f(j))

    for j in range(1, n_f):
        copy_ai(j).start()
    for a in range(2):
        for j in range(1, n_f):
            copy_a(a, j).start()

    def copy_b(a, j):
        return copy(xb.at[a, zl], xb.at[a, zl], sb.at[a, j], rb.at[a, j], zl_to=at_z(j))

    def copy_bi(j):
        return copy(info.at[zl], info.at[zl], sbi.at[j], rbi.at[j], zl_to=at_z(j))

    for j in range(1, n_f):
        copy_ai(j).wait_recv()
    for j in range(1, n_zl):
        copy_bi(j).start()
    for a in range(2):
        for j in range(1, n_f):
            copy_a(a, j).wait_recv()
        for j in range(1, n_zl):
            copy_b(a, j).start()

    for j in range(1, n_zl):
        copy_bi(j).wait_recv()
    table = info[...].reshape(col_tok, 128)
    slot = lax.broadcasted_iota(jnp.int32, (col_tok, slots), 1)
    token = lax.broadcasted_iota(jnp.int32, (col_tok, slots), 0)
    slot_expert = zl * n_xc + lax.shift_right_logical(slot, log2(n_src * CAP))
    slot_source = lax.shift_right_logical(slot, log2(CAP)) & (n_src - 1)
    slot_rank = (slot & (CAP - 1)).astype(F32)
    hit = [table[:, k : k + 1] == slot_expert for k in range(top)]
    named = functools.reduce(jnp.logical_or, hit)
    before_row = lax.broadcasted_iota(jnp.int32, (col_tok, col_tok), 0)
    before_col = lax.broadcasted_iota(jnp.int32, (col_tok, col_tok), 1)
    shift = log2(n_tok)
    earlier = (before_col < before_row) & (
        lax.shift_right_logical(before_col, shift) == lax.shift_right_logical(before_row, shift)
    )
    rank = dot(jnp.where(earlier, 1.0, 0.0).astype(BF16), jnp.where(named, 1.0, 0.0).astype(BF16), 1, 0)
    chosen = named & (rank == slot_rank) & (lax.shift_right_logical(token, shift) == slot_source)
    weight = jnp.zeros((col_tok, slots), F32)
    for k in range(top):
        value = table[:, top + k : top + k + 1].astype(F32) * (1.0 / 65536.0)
        weight = jnp.where(hit[k], value, weight)
    weight = jnp.where(chosen, weight, 0.0)
    high = weight.astype(BF16)
    w_hi[...] = high
    w_lo[...] = (weight - high.astype(F32)).astype(BF16)
    w_one[...] = jnp.where(chosen, 1.0, 0.0).astype(BF16)

    def copy_d(a, j):
        there = at_x(j)
        return copy(xs.at[a, there], xe.at[a, d, xc], sd.at[a, j], rd.at[a, j], xc_to=there)

    for a in range(2):
        for j in range(1, n_zl):
            copy_b(a, j).wait_recv()
        table_rows = xb[a].reshape(col_tok, cols)
        if a == 0:
            picked = dot(w_one[...], table_rows, 0, 0)
        else:
            picked = dot(w_hi[...], table_rows, 0, 0) + dot(w_lo[...], table_rows, 0, 0)
        xs[a] = picked.astype(BF16).reshape(n_xc, n_src * CAP, cols)
        xe[a, d, xc] = xs[a, xc]
        for j in range(1, n_xc):
            copy_d(a, j).start()

    def copy_e(a, j):
        return copy(xe.at[a, d], xe.at[a, d], se.at[a, j], re.at[a, j], d_to=at_d(j))

    for a in range(2):
        for j in range(1, n_xc):
            copy_d(a, j).wait_recv()
        for j in range(1, n_d):
            copy_e(a, j).start()

    def copy_r(k, j):
        there = at_f(j)
        return copy(rss.at[k, there], rsr.at[k, f], sr.at[k, j], rr.at[k, j], f_to=there)

    def from_d(k):
        return (d - k + n_d) % n_d

    @pl.loop(0, n_d)
    def _(k):
        chunk = from_d(k)

        @pl.when(k > 0)
        def _():
            for a in range(2):
                copy_e(a, k).wait_recv()

        x_rows = xe[0, chunk].reshape(rows, cols)
        pf[k, :, :hid] = dot(x_rows, wg_ref[...], 1, 0)
        pf[k, :, hid : 2 * hid] = dot(x_rows, wu_ref[...], 1, 0)
        pf[k, :, 2 * hid :] = dot(xe[1, chunk].reshape(rows, cols), wd_ref[...], 1, 1)
        rss[k] = pf[k].astype(BF16).reshape(n_f, part, 3 * hid)
        for j in range(1, n_f):
            copy_r(k, j).start()

    def copy_g(k, j):
        mine = agb.at[from_d(k), f]
        return copy(mine, mine, sg.at[k, j], rg.at[k, j], f_to=at_f(j))

    @pl.loop(0, n_d)
    def _(i):
        k = (i + 1) % n_d
        for j in range(1, n_f):
            copy_r(k, j).wait_recv()
        total = pf[k, pl.ds(pl.multiple_of(f * part, part), part), :]
        for j in range(1, n_f):
            total = total + rsr[k, at_f(j)].astype(F32)
        gate, up, grad = total[:, :hid], total[:, hid : 2 * hid], total[:, 2 * hid :]
        sigmoid = jax.nn.sigmoid(gate)
        swish = gate * sigmoid
        chunk = from_d(k)
        agb[chunk, f, :, :hid] = (swish * up).astype(BF16)
        agb[chunk, f, :, hid : 2 * hid] = (grad * up * sigmoid * (1.0 + gate * (1.0 - sigmoid))).astype(BF16)
        agb[chunk, f, :, 2 * hid :] = (grad * swish).astype(BF16)
        for j in range(1, n_f):
            copy_g(k, j).start()

    def products(k):
        values = agb[from_d(k)].reshape(rows, 3 * hid)
        out = dot(values[:, :hid], wd_ref[...], 1, 0)
        back = dot(values[:, hid : 2 * hid], wg_ref[...], 1, 1)
        return out, back + dot(values[:, 2 * hid :], wu_ref[...], 1, 1)

    def copy_h(k):
        return copy(hs.at[k], hr.at[k], sh.at[k], rh.at[k], d_to=from_d(k))

    @pl.loop(1, n_d)
    def _(k):
        for j in range(1, n_f):
            copy_g(k, j).wait_recv()
        out, back = products(k)
        hs[k, 0] = out.astype(BF16)
        hs[k, 1] = back.astype(BF16)
        copy_h(k).start()

    for j in range(1, n_f):
        copy_g(0, j).wait_recv()
    out, back = products(0)
    own[0] = out
    own[1] = back

    def copy_i(j):
        there = at_x(j)
        return copy(isb.at[there], irb.at[xc], si.at[j], ri.at[j], xc_to=there)

    for k in range(1, n_d):
        copy_h(k).wait_recv()
    for a in range(2):
        total = own[a]
        for k in range(1, n_d):
            total = total + hr[k, a].astype(F32)
        isb[:, a] = total.astype(BF16).reshape(n_xc, n_src * CAP, cols)
    irb[xc] = isb[xc]
    for j in range(1, n_xc):
        copy_i(j).start()

    all_values = agb[...].reshape(n_d * rows, 3 * hid)
    gdown_ref[...] = dot(all_values[:, :hid], xe[1].reshape(n_d * rows, cols), 0, 0)

    def copy_k(j):
        there = at_z(j)
        return copy(ks.at[there], kr.at[zl], sk.at[j], rk.at[j], zl_to=there)

    for j in range(1, n_xc):
        copy_i(j).wait_recv()
    returned = irb[:, 0].reshape(slots, cols)
    mixed_part = dot(w_hi[...], returned, 1, 0) + dot(w_lo[...], returned, 1, 0)
    grad_part = dot(w_one[...], irb[:, 1].reshape(slots, cols), 1, 0)
    for a, value in enumerate((mixed_part, grad_part)):
        value = value.reshape(n_zl, n_f * n_tok, cols)
        mp[:, a] = value
        ks[:, a] = value.astype(BF16)
    for j in range(1, n_zl):
        copy_k(j).start()

    ggate_ref[...] = dot(xe[0].reshape(n_d * rows, cols), all_values[:, hid : 2 * hid], 0, 0)

    def copy_l(j):
        there = at_f(j)
        return copy(ls.at[there], lr.at[f], sl.at[j], rl.at[j], f_to=there)

    for j in range(1, n_zl):
        copy_k(j).wait_recv()
    total = mp[zl]
    for j in range(1, n_zl):
        total = total + kr[at_z(j)].astype(F32)
    total = total.astype(BF16)
    for a in range(2):
        ls[:, a] = total[a].reshape(n_f, n_tok, cols)
    lr[f] = ls[f]
    for j in range(1, n_f):
        copy_l(j).start()

    gup_ref[...] = dot(xe[0].reshape(n_d * rows, cols), all_values[:, 2 * hid :], 0, 0)

    for j in range(1, n_f):
        copy_l(j).wait_recv()
    for owner in range(n_f):
        mixed_ref[:, owner * cols : (owner + 1) * cols] = lr[owner, 0]
        gtok_ref[:, owner * cols : (owner + 1) * cols] = lr[owner, 1]

    for j in range(1, n_f):
        copy_ai(j).wait_send()
        copy_l(j).wait_send()
        for a in range(2):
            copy_a(a, j).wait_send()
        for k in range(n_d):
            copy_r(k, j).wait_send()
            copy_g(k, j).wait_send()
    for j in range(1, n_zl):
        copy_bi(j).wait_send()
        copy_k(j).wait_send()
        for a in range(2):
            copy_b(a, j).wait_send()
    for j in range(1, n_xc):
        copy_i(j).wait_send()
        for a in range(2):
            copy_d(a, j).wait_send()
    for j in range(1, n_d):
        copy_h(j).wait_send()
        for a in range(2):
            copy_e(a, j).wait_send()


def body(sizes, tokens, routes, gate_fixed, gate_weight, up_weight, down_weight, cotangent):
    n_zl, n_xc, n_f, n_d = sizes
    n_tok, width = tokens.shape
    cols, hid = gate_weight.shape[1:]
    n_src = n_zl * n_f
    col_tok = n_src * n_tok
    slots = n_xc * n_src * CAP
    rows = slots
    part = rows // n_f
    vmem = pltpu.VMEM
    dma = pltpu.SemaphoreType.DMA
    outs = pl.pallas_call(
        functools.partial(kernel, sizes),
        out_shape=(
            jax.ShapeDtypeStruct((n_tok, width), BF16),
            jax.ShapeDtypeStruct((n_tok, width), BF16),
            jax.ShapeDtypeStruct((hid, cols), F32),
            jax.ShapeDtypeStruct((cols, hid), F32),
            jax.ShapeDtypeStruct((cols, hid), F32),
        ),
        in_specs=[pl.BlockSpec(memory_space=pltpu.VMEM)] * 7,
        out_specs=[pl.BlockSpec(memory_space=pltpu.VMEM)] * 5,
        scratch_shapes=[
            vmem((n_zl, n_f, n_tok, 128), jnp.int32),
            vmem((2, n_zl, n_f, n_tok, cols), BF16),
            vmem((2, n_xc, n_src * CAP, cols), BF16),
            vmem((2, n_d, n_xc, n_src * CAP, cols), BF16),
            vmem((n_d, rows, 3 * hid), F32),
            vmem((n_d, n_f, part, 3 * hid), BF16),
            vmem((n_d, n_f, part, 3 * hid), BF16),
            vmem((n_d, n_f, part, 3 * hid), BF16),
            vmem((n_d, 2, rows, cols), BF16),
            vmem((n_d, 2, rows, cols), BF16),
            vmem((2, rows, cols), F32),
            vmem((n_xc, 2, n_src * CAP, cols), BF16),
            vmem((n_xc, 2, n_src * CAP, cols), BF16),
            vmem((n_zl, 2, n_f * n_tok, cols), F32),
            vmem((n_zl, 2, n_f * n_tok, cols), BF16),
            vmem((n_zl, 2, n_f * n_tok, cols), BF16),
            vmem((n_f, 2, n_tok, cols), BF16),
            vmem((n_f, 2, n_tok, cols), BF16),
            vmem((col_tok, slots), BF16),
            vmem((col_tok, slots), BF16),
            vmem((col_tok, slots), BF16),
        ]
        + [dma((2, n_f)), dma((2, n_f)), dma((n_f,)), dma((n_f,))]
        + [dma((2, n_zl)), dma((2, n_zl)), dma((n_zl,)), dma((n_zl,))]
        + [dma((2, n_xc)), dma((2, n_xc)), dma((2, n_d)), dma((2, n_d))]
        + [dma((n_d, n_f))] * 4
        + [dma((n_d,))] * 2
        + [dma((n_xc,))] * 2
        + [dma((n_zl,))] * 2
        + [dma((n_f,))] * 2,
        compiler_params=pltpu.CompilerParams(
            collective_id=0, has_side_effects=True, vmem_limit_bytes=60 * 1024 * 1024
        ),
    )(tokens, cotangent, routes, gate_fixed, gate_weight[0], up_weight[0], down_weight[0])
    mixed, grad_tokens, grad_down, grad_gate, grad_up = outs
    return mixed, grad_tokens, grad_down[None], grad_gate[None], grad_up[None]


def solution(mesh):
    n_expert, n_f, n_d = (mesh.shape[name] for name in ("expert", "fsdp", "dp"))
    n_zl = 4 if n_expert >= 16 else 2
    sizes = (n_zl, n_expert // n_zl, n_f, n_d)
    tokens = P(("expert", "fsdp", "dp"), None)
    wide = P("expert", "fsdp", "dp")
    tall = P("expert", "dp", "fsdp")
    return jax.shard_map(
        functools.partial(body, sizes),
        mesh=mesh,
        in_specs=(tokens, tokens, tokens, wide, wide, tall, tokens),
        out_specs=(tokens, tokens, tall, wide, wide),
        check_vma=False,
    )
```

```python
import functools

import jax
import jax.numpy as jnp
from jax import lax
from jax.experimental import pallas as pl
from jax.experimental.pallas import tpu as pltpu
from jax.sharding import PartitionSpec as P

F32 = jnp.float32
BF16 = jnp.bfloat16
CAP = 2


def log2(number):
    assert number & (number - 1) == 0
    return number.bit_length() - 1


def dot(a, b, ca, cb):
    return lax.dot_general(a, b, (((ca,), (cb,)), ((), ())), preferred_element_type=F32)


def kernel(
    sizes,
    tok_ref, cot_ref, routes_ref, fixed_ref, wg_hbm, wu_hbm, wd_hbm,
    mixed_ref, gtok_ref, gdown_hbm, ggate_hbm, gup_hbm,
    wg_ref, wu_ref, wd_ref, gdown, ggate, gup,
    info, xb, xs, xe, pf, rss, r1, s2, r2, av, hs, hq, hr, own, isb, irb, mp, ks, kr, ls, lr, w_hi, w_lo, w_one,
    local_sem,
    sa, ra, sai, rai, sb, rb, sbi, rbi, sd, rd, se, re, sf, rf, sr, rr, sm, rm, sg, rg, sh, rh, sq, rq,
    si, ri, sk, rk, sl, rl,
):
    n_zl, n_xc, n_f, n_d = sizes
    n_tok, top = routes_ref.shape
    cols = wg_ref.shape[0]
    hid = wg_ref.shape[1]
    n_src = n_zl * n_f
    col_tok = n_src * n_tok
    slots = n_xc * n_src * CAP
    rows = slots
    part = rows // n_f
    half = n_xc // 2

    e = lax.axis_index("expert")
    f = lax.axis_index("fsdp")
    d = lax.axis_index("dp")
    zl = e // n_xc
    xc = e % n_xc

    def at_f(j):
        return (f + j) % n_f

    def at_z(j):
        return (zl + j) % n_zl

    def at_x(j):
        return (xc + j) % n_xc

    def at_d(j):
        return (d + j + n_d) % n_d

    def device(zl_to=zl, xc_to=xc, f_to=f, d_to=d):
        return {"expert": zl_to * n_xc + xc_to, "fsdp": f_to, "dp": d_to}

    sent = []

    def copy(src, dst, send, recv, **to):
        return pltpu.make_async_remote_copy(
            src_ref=src,
            dst_ref=dst,
            send_sem=send,
            recv_sem=recv,
            device_id=device(**to),
            device_id_type=pl.DeviceIdType.MESH,
        )

    def start(one):
        one.start()
        sent.append(one)

    def start_local(source, target, number):
        one = pltpu.make_async_copy(source, target, local_sem.at[number])
        one.start()
        return one

    barrier = pltpu.get_barrier_semaphore()
    count = 0
    for limit, name, at in ((n_f, "f_to", at_f), (n_zl, "zl_to", at_z), (n_xc, "xc_to", at_x), (n_d, "d_to", at_d)):
        for j in range(1, limit):
            pl.semaphore_signal(
                barrier, inc=1, device_id=device(**{name: at(j)}), device_id_type=pl.DeviceIdType.MESH
            )
            count += 1
    weights = [
        start_local(source, target, number)
        for number, (source, target) in enumerate(((wg_hbm, wg_ref), (wu_hbm, wu_ref), (wd_hbm, wd_ref)))
    ]

    lane = lax.broadcasted_iota(jnp.int32, (n_tok, 128), 1)
    packed = jnp.zeros((n_tok, 128), jnp.int32)
    for k in range(top):
        fixed = fixed_ref[:, k : k + 1]
        packed = jnp.where(lane == k, routes_ref[:, k : k + 1], packed)
        packed = jnp.where(lane == top + k, lax.shift_right_logical(fixed, 8), packed)
        packed = jnp.where(lane == 2 * top + k, fixed & 255, packed)
    info[zl, f] = packed.astype(F32).astype(BF16)
    own_cols = pl.ds(pl.multiple_of(f * cols, 128), cols)
    xb[0, zl, f] = tok_ref[:, own_cols]
    xb[1, zl, f] = cot_ref[:, own_cols]

    pl.semaphore_wait(barrier, count)

    def copy_a(a, j):
        there = at_f(j)
        src = (tok_ref, cot_ref)[a]
        columns = pl.ds(pl.multiple_of(there * cols, 128), cols)
        return copy(src.at[:, columns], xb.at[a, zl, f], sa.at[a, j], ra.at[a, j], f_to=there)

    def copy_ai(j):
        return copy(info.at[zl, f], info.at[zl, f], sai.at[j], rai.at[j], f_to=at_f(j))

    for j in range(1, n_f):
        start(copy_ai(j))
    for a in range(2):
        for j in range(1, n_f):
            start(copy_a(a, j))

    def copy_b(a, j):
        return copy(xb.at[a, zl], xb.at[a, zl], sb.at[a, j], rb.at[a, j], zl_to=at_z(j))

    def copy_bi(j):
        return copy(info.at[zl], info.at[zl], sbi.at[j], rbi.at[j], zl_to=at_z(j))

    for j in range(1, n_f):
        copy_ai(j).wait_recv()
    for j in range(1, n_zl):
        start(copy_bi(j))
    for a in range(2):
        for j in range(1, n_f):
            copy_a(a, j).wait_recv()
        for j in range(1, n_zl):
            start(copy_b(a, j))

    for j in range(1, n_zl):
        copy_bi(j).wait_recv()
    table = info[...].reshape(col_tok, 128).astype(F32)
    slot = lax.broadcasted_iota(jnp.int32, (col_tok, slots), 1)
    token = lax.broadcasted_iota(jnp.int32, (col_tok, slots), 0)
    slot_expert = (zl * n_xc + lax.shift_right_logical(slot, log2(n_src * CAP))).astype(F32)
    slot_source = lax.shift_right_logical(slot, log2(CAP)) & (n_src - 1)
    slot_rank = (slot & (CAP - 1)).astype(F32)
    hit = [table[:, k : k + 1] == slot_expert for k in range(top)]
    named = functools.reduce(jnp.logical_or, hit)
    before_row = lax.broadcasted_iota(jnp.int32, (col_tok, col_tok), 0)
    before_col = lax.broadcasted_iota(jnp.int32, (col_tok, col_tok), 1)
    shift = log2(n_tok)
    earlier = (before_col < before_row) & (
        lax.shift_right_logical(before_col, shift) == lax.shift_right_logical(before_row, shift)
    )
    rank = dot(jnp.where(earlier, 1.0, 0.0).astype(BF16), jnp.where(named, 1.0, 0.0).astype(BF16), 1, 0)
    chosen = named & (rank == slot_rank) & (lax.shift_right_logical(token, shift) == slot_source)
    weight = jnp.zeros((col_tok, slots), F32)
    for k in range(top):
        value = table[:, top + k : top + k + 1] * 256.0 + table[:, 2 * top + k : 2 * top + k + 1]
        weight = jnp.where(hit[k], value * (1.0 / 65536.0), weight)
    weight = jnp.where(chosen, weight, 0.0)
    high = weight.astype(BF16)
    w_hi[...] = high
    w_lo[...] = (weight - high.astype(F32)).astype(BF16)
    w_one[...] = jnp.where(chosen, 1.0, 0.0).astype(BF16)

    def copy_d(a, j):
        there = at_x(j)
        return copy(xs.at[a, there], xe.at[a, d, xc], sd.at[a, j], rd.at[a, j], xc_to=there)

    for a in range(2):
        for j in range(1, n_zl):
            copy_b(a, j).wait_recv()
        table_rows = xb[a].reshape(col_tok, cols)
        if a == 0:
            picked = dot(w_one[...], table_rows, 0, 0)
        else:
            picked = dot(w_hi[...], table_rows, 0, 0) + dot(w_lo[...], table_rows, 0, 0)
        xs[a] = picked.astype(BF16).reshape(n_xc, n_src * CAP, cols)
        xe[a, d, xc] = xs[a, xc]
        for j in range(1, n_xc):
            start(copy_d(a, j))

    def from_d(k):
        return at_d(-k)

    def copy_e(a, k):
        return copy(xe.at[a, d], xe.at[a, d], se.at[a, k], re.at[a, k], d_to=at_d(k))

    def copy_far(a, k):
        piece = xe.at[a, from_d(k), pl.ds(0, half) if k == 1 else pl.ds(half, half)]
        return copy(piece, piece, sf.at[a, k], rf.at[a, k], d_to=at_d(k))

    def send_e(a):
        for j in range(1, n_xc):
            copy_d(a, j).wait_recv()
        for k in (1, n_d - 1):
            start(copy_e(a, k))

    def take_e(a, k):
        if k == 2:
            for via in (1, n_d - 1):
                copy_far(a, via).wait_recv()
        elif k != 0:
            copy_e(a, k).wait_recv()
            start(copy_far(a, k))

    def sides(turn):
        step = 1 - 2 * ((f + turn) % 2)
        return (f + step + n_f) % n_f, (f - step + n_f) % n_f

    def sides_r(s, k):
        return sides(s if s < 2 else k % 2)

    def copy_r(s, k, which):
        first, _ = sides_r(s, k)
        quarter = at_f(2) if which == 0 else first
        return copy(
            rss.at[s, k, quarter], r1.at[s, k, quarter], sr.at[s, k, which], rr.at[s, k, which], f_to=first
        )

    def copy_m(s, k):
        _, second = sides_r(s, k)
        return copy(s2.at[s, k], r2.at[s, k], sm.at[s, k], rm.at[s, k], f_to=second)

    def part_of(quarter):
        return pl.ds(pl.multiple_of(quarter * part, part), part)

    def scatter(s, k):
        operand = xe[0 if s < 2 else 1, from_d(k)].reshape(rows, cols)
        product = dot(operand, (wg_ref, wu_ref, wd_ref)[s][...], 1, 0 if s < 2 else 1)
        pf[s, k] = product
        rss[s, k] = product.astype(BF16).reshape(n_f, part, hid)
        for which in range(2):
            start(copy_r(s, k, which))

    def scatter_more(k):
        for s in range(3):
            copy_r(s, k, 0).wait_recv()
            _, second = sides_r(s, k)
            s2[s, k] = (pf[s, k, part_of(second), :] + r1[s, k, second].astype(F32)).astype(BF16)
            start(copy_m(s, k))

    def total_of(s, k):
        copy_r(s, k, 1).wait_recv()
        copy_m(s, k).wait_recv()
        return pf[s, k, part_of(f), :] + r1[s, k, f].astype(F32) + r2[s, k].astype(F32)

    def copy_g(s, k, which):
        first, second = sides(k % 2 if s == 0 else s - 1)
        mine = av.at[s, from_d(k), second if which == 2 else f]
        return copy(mine, mine, sg.at[s, k, which], rg.at[s, k, which], f_to=second if which == 0 else first)

    def gather(k):
        gate = total_of(0, k)
        up = total_of(1, k)
        sigmoid = jax.nn.sigmoid(gate)
        swish = gate * sigmoid
        av[0, from_d(k), f] = (swish * up).astype(BF16)
        for which in range(2):
            start(copy_g(0, k, which))
        grad = total_of(2, k)
        av[1, from_d(k), f] = (grad * up * sigmoid * (1.0 + gate * (1.0 - sigmoid))).astype(BF16)
        av[2, from_d(k), f] = (grad * swish).astype(BF16)
        for which in range(2):
            for s in (1, 2):
                start(copy_g(s, k, which))

    def gather_more(k):
        for s in range(3):
            copy_g(s, k, 0).wait_recv()
            start(copy_g(s, k, 2))

    def copy_h(a, k):
        return copy(hs.at[a, k], hr.at[a, k], sh.at[a, k], rh.at[a, k], d_to=from_d(k))

    def half_of(via):
        return pl.ds(0, half) if via == 1 else pl.ds(half, half)

    def copy_half(a, via):
        return copy(hs.at[a, 2, half_of(via)], hq.at[a, 0 if via == 1 else 1], sh.at[a, 0 if via == 1 else 2],
                    rh.at[a, 0 if via == 1 else 2], d_to=at_d(via))

    def copy_on(a, via):
        number = 0 if via == 1 else 1
        return copy(hq.at[a, number], hr.at[a, 2, half_of(via)], sq.at[a, number], rq.at[a, number], d_to=at_d(via))

    def product_of(a, k):
        for s in (0,) if a == 0 else (1, 2):
            for which in (1, 2):
                copy_g(s, k, which).wait_recv()
        chunk = from_d(k)
        if a == 0:
            return dot(av[0, chunk].reshape(rows, hid), wd_ref[...], 1, 0)
        back = dot(av[1, chunk].reshape(rows, hid), wg_ref[...], 1, 1)
        return back + dot(av[2, chunk].reshape(rows, hid), wu_ref[...], 1, 1)

    def output(a, k):
        hs[a, k] = product_of(a, k).astype(BF16).reshape(n_xc, n_src * CAP, cols)
        if k == 2:
            for via in (1, n_d - 1):
                start(copy_half(a, via))
        else:
            start(copy_h(a, k))

    def pass_on(a):
        for via in (1, n_d - 1):
            copy_half(a, via).wait_recv()
            start(copy_on(a, via))

    def copy_i(a, j):
        there = at_x(j)
        return copy(isb.at[a, there], irb.at[a, xc], si.at[a, j], ri.at[a, j], xc_to=there)

    def send_i(a):
        own[...] = product_of(a, 0)
        for k in (1, n_d - 1):
            copy_h(a, k).wait_recv()
        for via in (1, n_d - 1):
            copy_on(a, via).wait_recv()
        total = own[...].reshape(n_xc, n_src * CAP, cols)
        for k in range(1, n_d):
            total = total + hr[a, k].astype(F32)
        isb[a] = total.astype(BF16)
        irb[a, xc] = isb[a, xc]
        for j in range(1, n_xc):
            start(copy_i(a, j))

    def copy_k(a, j):
        there = at_z(j)
        return copy(ks.at[a, there], kr.at[a, zl], sk.at[a, j], rk.at[a, j], zl_to=there)

    def send_k(a):
        for j in range(1, n_xc):
            copy_i(a, j).wait_recv()
        returned = irb[a].reshape(slots, cols)
        if a == 0:
            value = dot(w_hi[...], returned, 1, 0) + dot(w_lo[...], returned, 1, 0)
        else:
            value = dot(w_one[...], returned, 1, 0)
        value = value.reshape(n_zl, n_f * n_tok, cols)
        mp[a] = value
        ks[a] = value.astype(BF16)
        for j in range(1, n_zl):
            start(copy_k(a, j))

    def copy_l(a, j):
        there = at_f(j)
        return copy(ls.at[a, there], lr.at[a, f], sl.at[a, j], rl.at[a, j], f_to=there)

    def send_l(a):
        for j in range(1, n_zl):
            copy_k(a, j).wait_recv()
        total = mp[a, zl]
        for j in range(1, n_zl):
            total = total + kr[a, at_z(j)].astype(F32)
        ls[a] = total.astype(BF16).reshape(n_f, n_tok, cols)
        lr[a, f] = ls[a, f]
        for j in range(1, n_f):
            start(copy_l(a, j))

    def finish(a):
        for j in range(1, n_f):
            copy_l(a, j).wait_recv()
        for owner in range(n_f):
            (mixed_ref, gtok_ref)[a][:, owner * cols : (owner + 1) * cols] = lr[a, owner]

    for one in weights:
        one.wait()
    send_e(0)
    scatter(0, 0)
    scatter(1, 0)
    send_e(1)
    scatter(2, 0)
    for k, previous in ((1, 0), (3, 1), (2, 3)):
        take_e(0, k)
        scatter(0, k)
        scatter(1, k)
        take_e(1, k)
        scatter(2, k)
        scatter_more(previous)
    gather(1)
    scatter_more(2)
    gather_more(1)
    gather(3)
    gather(2)
    gather_more(3)
    gather(0)
    output(0, 1)
    output(1, 1)
    gather_more(2)
    output(0, 3)
    output(1, 3)
    gather_more(0)
    output(0, 2)
    output(1, 2)
    pass_on(0)
    send_i(0)
    pass_on(1)
    send_i(1)
    all_rows = n_d * rows
    gdown[...] = dot(av[0].reshape(all_rows, hid), xe[1].reshape(all_rows, cols), 0, 0)
    results = [start_local(gdown, gdown_hbm, 0)]
    send_k(0)
    send_k(1)
    ggate[...] = dot(xe[0].reshape(all_rows, cols), av[1].reshape(all_rows, hid), 0, 0)
    results.append(start_local(ggate, ggate_hbm, 1))
    send_l(0)
    send_l(1)
    gup[...] = dot(xe[0].reshape(all_rows, cols), av[2].reshape(all_rows, hid), 0, 0)
    results.append(start_local(gup, gup_hbm, 2))
    finish(0)
    finish(1)
    for one in sent:
        one.wait_send()
    for one in results:
        one.wait()


def body(sizes, tokens, routes, gate_fixed, gate_weight, up_weight, down_weight, cotangent):
    n_zl, n_xc, n_f, n_d = sizes
    n_tok, width = tokens.shape
    cols, hid = gate_weight.shape[1:]
    n_src = n_zl * n_f
    col_tok = n_src * n_tok
    slots = n_xc * n_src * CAP
    rows = slots
    part = rows // n_f
    vmem = pltpu.VMEM
    dma = pltpu.SemaphoreType.DMA
    outs = pl.pallas_call(
        functools.partial(kernel, sizes),
        out_shape=(
            jax.ShapeDtypeStruct((n_tok, width), BF16),
            jax.ShapeDtypeStruct((n_tok, width), BF16),
            jax.ShapeDtypeStruct((hid, cols), F32),
            jax.ShapeDtypeStruct((cols, hid), F32),
            jax.ShapeDtypeStruct((cols, hid), F32),
        ),
        in_specs=[pl.BlockSpec(memory_space=pltpu.VMEM)] * 4 + [pl.BlockSpec(memory_space=pl.ANY)] * 3,
        out_specs=[pl.BlockSpec(memory_space=pltpu.VMEM)] * 2 + [pl.BlockSpec(memory_space=pl.ANY)] * 3,
        scratch_shapes=[
            vmem((cols, hid), BF16),
            vmem((cols, hid), BF16),
            vmem((hid, cols), BF16),
            vmem((hid, cols), F32),
            vmem((cols, hid), F32),
            vmem((cols, hid), F32),
            vmem((n_zl, n_f, n_tok, 128), BF16),
            vmem((2, n_zl, n_f, n_tok, cols), BF16),
            vmem((2, n_xc, n_src * CAP, cols), BF16),
            vmem((2, n_d, n_xc, n_src * CAP, cols), BF16),
            vmem((3, n_d, rows, hid), F32),
            vmem((3, n_d, n_f, part, hid), BF16),
            vmem((3, n_d, n_f, part, hid), BF16),
            vmem((3, n_d, part, hid), BF16),
            vmem((3, n_d, part, hid), BF16),
            vmem((3, n_d, n_f, part, hid), BF16),
            vmem((2, n_d, n_xc, n_src * CAP, cols), BF16),
            vmem((2, 2, n_xc // 2, n_src * CAP, cols), BF16),
            vmem((2, n_d, n_xc, n_src * CAP, cols), BF16),
            vmem((rows, cols), F32),
            vmem((2, n_xc, n_src * CAP, cols), BF16),
            vmem((2, n_xc, n_src * CAP, cols), BF16),
            vmem((2, n_zl, n_f * n_tok, cols), F32),
            vmem((2, n_zl, n_f * n_tok, cols), BF16),
            vmem((2, n_zl, n_f * n_tok, cols), BF16),
            vmem((2, n_f, n_tok, cols), BF16),
            vmem((2, n_f, n_tok, cols), BF16),
            vmem((col_tok, slots), BF16),
            vmem((col_tok, slots), BF16),
            vmem((col_tok, slots), BF16),
            dma((3,)),
        ]
        + [dma((2, n_f)), dma((2, n_f)), dma((n_f,)), dma((n_f,))]
        + [dma((2, n_zl)), dma((2, n_zl)), dma((n_zl,)), dma((n_zl,))]
        + [dma((2, n_xc)), dma((2, n_xc))]
        + [dma((2, n_d))] * 4
        + [dma((3, n_d, 2))] * 2
        + [dma((3, n_d))] * 2
        + [dma((3, n_d, 3))] * 2
        + [dma((2, n_d))] * 2
        + [dma((2, 2))] * 2
        + [dma((2, n_xc))] * 2
        + [dma((2, n_zl))] * 2
        + [dma((2, n_f))] * 2,
        compiler_params=pltpu.CompilerParams(
            collective_id=0, has_side_effects=True, vmem_limit_bytes=60 * 1024 * 1024
        ),
    )(tokens, cotangent, routes, gate_fixed, gate_weight[0], up_weight[0], down_weight[0])
    mixed, grad_tokens, grad_down, grad_gate, grad_up = outs
    return mixed, grad_tokens, grad_down[None], grad_gate[None], grad_up[None]


def solution(mesh):
    n_expert, n_f, n_d = (mesh.shape[name] for name in ("expert", "fsdp", "dp"))
    n_zl = 4 if n_expert >= 16 else 2
    sizes = (n_zl, n_expert // n_zl, n_f, n_d)
    tokens = P(("expert", "fsdp", "dp"), None)
    wide = P("expert", "fsdp", "dp")
    tall = P("expert", "dp", "fsdp")
    return jax.shard_map(
        functools.partial(body, sizes),
        mesh=mesh,
        in_specs=(tokens, tokens, tokens, wide, wide, tall, tokens),
        out_specs=(tokens, tokens, tall, wide, wide),
        check_vma=False,
    )
```

```python
import functools

import jax
import jax.numpy as jnp
from jax import lax
from jax.experimental import pallas as pl
from jax.experimental.pallas import tpu as pltpu
from jax.sharding import PartitionSpec as P

F32 = jnp.float32
BF16 = jnp.bfloat16
CAP = 2


def log2(number):
    assert number & (number - 1) == 0
    return number.bit_length() - 1


def dot(a, b, ca, cb):
    return lax.dot_general(a, b, (((ca,), (cb,)), ((), ())), preferred_element_type=F32)


def kernel(
    sizes,
    tok_ref, cot_ref, routes_ref, fixed_ref, wg_hbm, wu_hbm, wd_hbm,
    mixed_ref, gtok_ref, gdown_hbm, ggate_hbm, gup_hbm,
    wg_ref, wu_ref, wd_ref, gdown, ggate, gup,
    info, xb, xs, xe, pf, rss, r1, s2, r2, av, hs, hq, hr, own, isb, irb, mp, ks, kr, ls, lr, w_hi, w_lo, w_one,
    local_sem,
    sa, ra, sai, rai, sb, rb, sbi, rbi, sd, rd, se, re, sf, rf, sr, rr, sm, rm, sg, rg, sh, rh, sq, rq,
    si, ri, sk, rk, sl, rl,
):
    n_zl, n_xc, n_f, n_d = sizes
    top, n_tok = routes_ref.shape
    cols = wg_ref.shape[0]
    hid = wg_ref.shape[1]
    n_src = n_zl * n_f
    col_tok = n_src * n_tok
    slots = n_xc * n_src * CAP
    rows = slots
    part = rows // n_f
    half = n_xc // 2

    e = lax.axis_index("expert")
    f = lax.axis_index("fsdp")
    d = lax.axis_index("dp")
    zl = e // n_xc
    xc = e % n_xc

    def at_f(j):
        return (f + j) % n_f

    def at_z(j):
        return (zl + j) % n_zl

    def at_x(j):
        return (xc + j) % n_xc

    def at_d(j):
        return (d + j + n_d) % n_d

    def device(zl_to=zl, xc_to=xc, f_to=f, d_to=d):
        return {"expert": zl_to * n_xc + xc_to, "fsdp": f_to, "dp": d_to}

    sent = []

    def copy(src, dst, send, recv, **to):
        return pltpu.make_async_remote_copy(
            src_ref=src,
            dst_ref=dst,
            send_sem=send,
            recv_sem=recv,
            device_id=device(**to),
            device_id_type=pl.DeviceIdType.MESH,
        )

    def start(one):
        one.start()
        sent.append(one)

    def start_local(source, target, number):
        one = pltpu.make_async_copy(source, target, local_sem.at[number])
        one.start()
        return one

    barrier = pltpu.get_barrier_semaphore()
    count = 0
    for limit, name, at in ((n_f, "f_to", at_f), (n_zl, "zl_to", at_z), (n_xc, "xc_to", at_x), (n_d, "d_to", at_d)):
        for j in range(1, limit):
            pl.semaphore_signal(
                barrier, inc=1, device_id=device(**{name: at(j)}), device_id_type=pl.DeviceIdType.MESH
            )
            count += 1
    weights = [
        start_local(source, target, number)
        for number, (source, target) in enumerate(((wg_hbm, wg_ref), (wu_hbm, wu_ref), (wd_hbm, wd_ref)))
    ]

    lane = lax.broadcasted_iota(jnp.int32, (n_tok, 128), 1)
    eye = lax.broadcasted_iota(jnp.int32, (n_tok, n_tok), 0) == lax.broadcasted_iota(jnp.int32, (n_tok, n_tok), 1)
    chosen_ids, fixed = routes_ref[...], fixed_ref[...]
    packed = jnp.zeros((n_tok, 128), F32)
    for number, values in enumerate((chosen_ids, lax.shift_right_logical(fixed, 8), fixed & 255)):
        values = values.astype(F32)
        for k in range(top):
            column = jnp.sum(jnp.where(eye, values[k : k + 1, :], 0.0), axis=1, keepdims=True)
            packed = jnp.where(lane == number * top + k, column, packed)
    info[zl, f] = packed.astype(BF16)
    own_cols = pl.ds(pl.multiple_of(f * cols, 128), cols)
    xb[0, zl, f] = tok_ref[:, own_cols]
    xb[1, zl, f] = cot_ref[:, own_cols]

    pl.semaphore_wait(barrier, count)

    def copy_a(a, j):
        there = at_f(j)
        src = (tok_ref, cot_ref)[a]
        columns = pl.ds(pl.multiple_of(there * cols, 128), cols)
        return copy(src.at[:, columns], xb.at[a, zl, f], sa.at[a, j], ra.at[a, j], f_to=there)

    def copy_ai(j):
        return copy(info.at[zl, f], info.at[zl, f], sai.at[j], rai.at[j], f_to=at_f(j))

    for j in range(1, n_f):
        start(copy_ai(j))
    for a in range(2):
        for j in range(1, n_f):
            start(copy_a(a, j))

    def copy_b(a, j):
        return copy(xb.at[a, zl], xb.at[a, zl], sb.at[a, j], rb.at[a, j], zl_to=at_z(j))

    def copy_bi(j):
        return copy(info.at[zl], info.at[zl], sbi.at[j], rbi.at[j], zl_to=at_z(j))

    for j in range(1, n_f):
        copy_ai(j).wait_recv()
    for j in range(1, n_zl):
        start(copy_bi(j))
    for a in range(2):
        for j in range(1, n_f):
            copy_a(a, j).wait_recv()
        for j in range(1, n_zl):
            start(copy_b(a, j))

    for j in range(1, n_zl):
        copy_bi(j).wait_recv()
    table = info[...].reshape(col_tok, 128).astype(F32)
    slot = lax.broadcasted_iota(jnp.int32, (col_tok, slots), 1)
    token = lax.broadcasted_iota(jnp.int32, (col_tok, slots), 0)
    slot_expert = (zl * n_xc + lax.shift_right_logical(slot, log2(n_src * CAP))).astype(F32)
    slot_source = lax.shift_right_logical(slot, log2(CAP)) & (n_src - 1)
    slot_rank = (slot & (CAP - 1)).astype(F32)
    hit = [table[:, k : k + 1] == slot_expert for k in range(top)]
    named = functools.reduce(jnp.logical_or, hit)
    before_row = lax.broadcasted_iota(jnp.int32, (col_tok, col_tok), 0)
    before_col = lax.broadcasted_iota(jnp.int32, (col_tok, col_tok), 1)
    shift = log2(n_tok)
    earlier = (before_col < before_row) & (
        lax.shift_right_logical(before_col, shift) == lax.shift_right_logical(before_row, shift)
    )
    rank = dot(jnp.where(earlier, 1.0, 0.0).astype(BF16), jnp.where(named, 1.0, 0.0).astype(BF16), 1, 0)
    chosen = named & (rank == slot_rank) & (lax.shift_right_logical(token, shift) == slot_source)
    weight = jnp.zeros((col_tok, slots), F32)
    for k in range(top):
        value = table[:, top + k : top + k + 1] * 256.0 + table[:, 2 * top + k : 2 * top + k + 1]
        weight = jnp.where(hit[k], value * (1.0 / 65536.0), weight)
    weight = jnp.where(chosen, weight, 0.0)
    high = weight.astype(BF16)
    w_hi[...] = high
    w_lo[...] = (weight - high.astype(F32)).astype(BF16)
    w_one[...] = jnp.where(chosen, 1.0, 0.0).astype(BF16)

    def copy_d(a, j):
        there = at_x(j)
        return copy(xs.at[a, there], xe.at[a, d, xc], sd.at[a, j], rd.at[a, j], xc_to=there)

    def send_d(a):
        for j in range(1, n_zl):
            copy_b(a, j).wait_recv()
        table_rows = xb[a].reshape(col_tok, cols)
        if a == 0:
            picked = dot(w_one[...], table_rows, 0, 0)
        else:
            picked = dot(w_hi[...], table_rows, 0, 0) + dot(w_lo[...], table_rows, 0, 0)
        xs[a] = picked.astype(BF16).reshape(n_xc, n_src * CAP, cols)
        xe[a, d, xc] = xs[a, xc]
        for j in range(1, n_xc):
            start(copy_d(a, j))

    def from_d(k):
        return at_d(-k)

    def copy_e(a, k):
        return copy(xe.at[a, d], xe.at[a, d], se.at[a, k], re.at[a, k], d_to=at_d(k))

    def copy_far(a, k):
        piece = xe.at[a, from_d(k), pl.ds(0, half) if k == 1 else pl.ds(half, half)]
        return copy(piece, piece, sf.at[a, k], rf.at[a, k], d_to=at_d(k))

    def send_e(a):
        for j in range(1, n_xc):
            copy_d(a, j).wait_recv()
        for k in (1, n_d - 1):
            start(copy_e(a, k))

    def take_e(a, k):
        if k == 2:
            for via in (1, n_d - 1):
                copy_far(a, via).wait_recv()
        elif k != 0:
            copy_e(a, k).wait_recv()
            start(copy_far(a, k))

    def sides(turn):
        step = 1 - 2 * ((f + turn) % 2)
        return (f + step + n_f) % n_f, (f - step + n_f) % n_f

    def sides_r(s, k):
        return sides(s if s < 2 else k % 2)

    def copy_r(s, k, which):
        first, _ = sides_r(s, k)
        quarter = at_f(2) if which == 0 else first
        return copy(
            rss.at[s, k, quarter], r1.at[s, k, quarter], sr.at[s, k, which], rr.at[s, k, which], f_to=first
        )

    def copy_m(s, k):
        _, second = sides_r(s, k)
        return copy(s2.at[s, k], r2.at[s, k], sm.at[s, k], rm.at[s, k], f_to=second)

    def part_of(quarter):
        return pl.ds(pl.multiple_of(quarter * part, part), part)

    def scatter(s, k):
        operand = xe[0 if s < 2 else 1, from_d(k)].reshape(rows, cols)
        product = dot(operand, (wg_ref, wu_ref, wd_ref)[s][...], 1, 0 if s < 2 else 1)
        pf[s, k] = product
        rss[s, k] = product.astype(BF16).reshape(n_f, part, hid)
        for which in range(2):
            start(copy_r(s, k, which))

    def scatter_more(s, k):
        copy_r(s, k, 0).wait_recv()
        _, second = sides_r(s, k)
        s2[s, k] = (pf[s, k, part_of(second), :] + r1[s, k, second].astype(F32)).astype(BF16)
        start(copy_m(s, k))

    def total_of(s, k):
        copy_r(s, k, 1).wait_recv()
        copy_m(s, k).wait_recv()
        return pf[s, k, part_of(f), :] + r1[s, k, f].astype(F32) + r2[s, k].astype(F32)

    def copy_g(s, k, which):
        first, second = sides(k % 2 if s == 0 else s - 1)
        mine = av.at[s, from_d(k), second if which == 2 else f]
        return copy(mine, mine, sg.at[s, k, which], rg.at[s, k, which], f_to=second if which == 0 else first)

    def activations(k):
        gate = pf[0, k, part_of(f), :]
        sigmoid = jax.nn.sigmoid(gate)
        return gate, pf[1, k, part_of(f), :], sigmoid, gate * sigmoid

    def gather_hidden(k):
        for s in range(2):
            pf[s, k, part_of(f), :] = total_of(s, k)
        _, up, _, swish = activations(k)
        av[0, from_d(k), f] = (swish * up).astype(BF16)
        for which in range(2):
            start(copy_g(0, k, which))

    def gather_grads(k):
        grad = total_of(2, k)
        gate, up, sigmoid, swish = activations(k)
        av[1, from_d(k), f] = (grad * up * sigmoid * (1.0 + gate * (1.0 - sigmoid))).astype(BF16)
        av[2, from_d(k), f] = (grad * swish).astype(BF16)
        for which in range(2):
            for s in (1, 2):
                start(copy_g(s, k, which))

    def gather_more(a, k):
        for s in (0,) if a == 0 else (1, 2):
            copy_g(s, k, 0).wait_recv()
            start(copy_g(s, k, 2))

    def copy_h(a, k):
        return copy(hs.at[a, k], hr.at[a, k], sh.at[a, k], rh.at[a, k], d_to=from_d(k))

    def half_of(via):
        return pl.ds(0, half) if via == 1 else pl.ds(half, half)

    def copy_half(a, via):
        return copy(hs.at[a, 2, half_of(via)], hq.at[a, 0 if via == 1 else 1], sh.at[a, 0 if via == 1 else 2],
                    rh.at[a, 0 if via == 1 else 2], d_to=at_d(via))

    def copy_on(a, via):
        number = 0 if via == 1 else 1
        return copy(hq.at[a, number], hr.at[a, 2, half_of(via)], sq.at[a, number], rq.at[a, number], d_to=at_d(via))

    def product_of(a, k):
        for s in (0,) if a == 0 else (1, 2):
            for which in (1, 2):
                copy_g(s, k, which).wait_recv()
        chunk = from_d(k)
        if a == 0:
            return dot(av[0, chunk].reshape(rows, hid), wd_ref[...], 1, 0)
        back = dot(av[1, chunk].reshape(rows, hid), wg_ref[...], 1, 1)
        return back + dot(av[2, chunk].reshape(rows, hid), wu_ref[...], 1, 1)

    def output(a, k):
        hs[a, k] = product_of(a, k).astype(BF16).reshape(n_xc, n_src * CAP, cols)
        if k == 2:
            for via in (1, n_d - 1):
                start(copy_half(a, via))
        else:
            start(copy_h(a, k))

    def pass_on(a):
        for via in (1, n_d - 1):
            copy_half(a, via).wait_recv()
            start(copy_on(a, via))

    def copy_i(a, j):
        there = at_x(j)
        return copy(isb.at[a, there], irb.at[a, xc], si.at[a, j], ri.at[a, j], xc_to=there)

    def send_i(a):
        own[...] = product_of(a, 0)
        for k in (1, n_d - 1):
            copy_h(a, k).wait_recv()
        for via in (1, n_d - 1):
            copy_on(a, via).wait_recv()
        total = own[...].reshape(n_xc, n_src * CAP, cols)
        for k in range(1, n_d):
            total = total + hr[a, k].astype(F32)
        isb[a] = total.astype(BF16)
        irb[a, xc] = isb[a, xc]
        for j in range(1, n_xc):
            start(copy_i(a, j))

    def copy_k(a, j):
        there = at_z(j)
        return copy(ks.at[a, there], kr.at[a, zl], sk.at[a, j], rk.at[a, j], zl_to=there)

    def send_k(a):
        for j in range(1, n_xc):
            copy_i(a, j).wait_recv()
        returned = irb[a].reshape(slots, cols)
        if a == 0:
            value = dot(w_hi[...], returned, 1, 0) + dot(w_lo[...], returned, 1, 0)
        else:
            value = dot(w_one[...], returned, 1, 0)
        value = value.reshape(n_zl, n_f * n_tok, cols)
        mp[a] = value
        ks[a] = value.astype(BF16)
        for j in range(1, n_zl):
            start(copy_k(a, j))

    def copy_l(a, j):
        there = at_f(j)
        return copy(ls.at[a, there], lr.at[a, f], sl.at[a, j], rl.at[a, j], f_to=there)

    def send_l(a):
        for j in range(1, n_zl):
            copy_k(a, j).wait_recv()
        total = mp[a, zl]
        for j in range(1, n_zl):
            total = total + kr[a, at_z(j)].astype(F32)
        ls[a] = total.astype(BF16).reshape(n_f, n_tok, cols)
        lr[a, f] = ls[a, f]
        for j in range(1, n_f):
            start(copy_l(a, j))

    def finish(a):
        for j in range(1, n_f):
            copy_l(a, j).wait_recv()
        for owner in range(n_f):
            (mixed_ref, gtok_ref)[a][:, owner * cols : (owner + 1) * cols] = lr[a, owner]

    send_d(0)
    for one in weights:
        one.wait()
    send_e(0)
    scatter(0, 0)
    scatter(1, 0)
    send_d(1)
    send_e(1)
    scatter(2, 0)
    take_e(0, 1)
    scatter(0, 1)
    scatter(1, 1)
    scatter_more(0, 0)
    scatter_more(1, 0)
    take_e(0, 3)
    scatter(0, 3)
    scatter(1, 3)
    take_e(1, 1)
    scatter(2, 1)
    scatter_more(2, 0)
    scatter_more(0, 1)
    scatter_more(1, 1)
    take_e(1, 3)
    scatter(2, 3)
    take_e(0, 2)
    scatter(0, 2)
    scatter(1, 2)
    scatter_more(2, 1)
    scatter_more(0, 3)
    scatter_more(1, 3)
    take_e(1, 2)
    scatter(2, 2)
    scatter_more(2, 3)
    gather_hidden(1)
    for s in range(3):
        scatter_more(s, 2)
    gather_hidden(3)
    gather_more(0, 1)
    gather_hidden(0)
    gather_hidden(2)
    gather_more(0, 3)
    gather_grads(2)
    output(0, 1)
    gather_more(0, 0)
    gather_more(0, 2)
    output(0, 3)
    gather_grads(1)
    output(0, 2)
    gather_more(1, 2)
    gather_grads(3)
    pass_on(0)
    gather_more(1, 1)
    gather_grads(0)
    output(1, 2)
    send_i(0)
    gather_more(1, 3)
    output(1, 1)
    pass_on(1)
    gather_more(1, 0)
    output(1, 3)
    send_k(0)
    send_i(1)
    all_rows = n_d * rows
    gdown[...] = dot(av[0].reshape(all_rows, hid), xe[1].reshape(all_rows, cols), 0, 0)
    results = [start_local(gdown, gdown_hbm, 0)]
    send_l(0)
    send_k(1)
    ggate[...] = dot(xe[0].reshape(all_rows, cols), av[1].reshape(all_rows, hid), 0, 0)
    results.append(start_local(ggate, ggate_hbm, 1))
    finish(0)
    send_l(1)
    gup[...] = dot(xe[0].reshape(all_rows, cols), av[2].reshape(all_rows, hid), 0, 0)
    results.append(start_local(gup, gup_hbm, 2))
    finish(1)
    for one in sent:
        one.wait_send()
    for one in results:
        one.wait()


def hand_over_kernel(*refs):
    count = (len(refs) - 1) // 3
    sources, targets, held, sem = refs[:count], refs[count : 2 * count], refs[2 * count : 3 * count], refs[-1]
    into = [pltpu.make_async_copy(sources[i], held[i], sem.at[0, i]) for i in range(count)]
    out = [pltpu.make_async_copy(held[i], targets[i], sem.at[1, i]) for i in range(count)]
    for one in into:
        one.start()
    for i in range(count):
        into[i].wait()
        out[i].start()
    for one in out:
        one.wait()


def hand_over(arrays):
    anywhere = pl.BlockSpec(memory_space=pl.ANY)
    return pl.pallas_call(
        hand_over_kernel,
        out_shape=tuple(jax.ShapeDtypeStruct(one.shape, one.dtype) for one in arrays),
        in_specs=[anywhere] * len(arrays),
        out_specs=[anywhere] * len(arrays),
        scratch_shapes=[pltpu.VMEM(one.shape, one.dtype) for one in arrays]
        + [pltpu.SemaphoreType.DMA((2, len(arrays)))],
    )(*arrays)


def body(sizes, tokens, routes, gate_fixed, gate_weight, up_weight, down_weight, cotangent):
    n_zl, n_xc, n_f, n_d = sizes
    n_tok, width = tokens.shape
    cols, hid = gate_weight.shape[1:]
    n_src = n_zl * n_f
    col_tok = n_src * n_tok
    slots = n_xc * n_src * CAP
    rows = slots
    part = rows // n_f
    vmem = pltpu.VMEM
    dma = pltpu.SemaphoreType.DMA
    outs = pl.pallas_call(
        functools.partial(kernel, sizes),
        out_shape=(
            jax.ShapeDtypeStruct((n_tok, width), BF16),
            jax.ShapeDtypeStruct((n_tok, width), BF16),
            jax.ShapeDtypeStruct((hid, cols), F32),
            jax.ShapeDtypeStruct((cols, hid), F32),
            jax.ShapeDtypeStruct((cols, hid), F32),
        ),
        in_specs=[pl.BlockSpec(memory_space=pltpu.VMEM)] * 4 + [pl.BlockSpec(memory_space=pl.ANY)] * 3,
        out_specs=[pl.BlockSpec(memory_space=pltpu.VMEM)] * 2 + [pl.BlockSpec(memory_space=pl.ANY)] * 3,
        scratch_shapes=[
            vmem((cols, hid), BF16),
            vmem((cols, hid), BF16),
            vmem((hid, cols), BF16),
            vmem((hid, cols), F32),
            vmem((cols, hid), F32),
            vmem((cols, hid), F32),
            vmem((n_zl, n_f, n_tok, 128), BF16),
            vmem((2, n_zl, n_f, n_tok, cols), BF16),
            vmem((2, n_xc, n_src * CAP, cols), BF16),
            vmem((2, n_d, n_xc, n_src * CAP, cols), BF16),
            vmem((3, n_d, rows, hid), F32),
            vmem((3, n_d, n_f, part, hid), BF16),
            vmem((3, n_d, n_f, part, hid), BF16),
            vmem((3, n_d, part, hid), BF16),
            vmem((3, n_d, part, hid), BF16),
            vmem((3, n_d, n_f, part, hid), BF16),
            vmem((2, n_d, n_xc, n_src * CAP, cols), BF16),
            vmem((2, 2, n_xc // 2, n_src * CAP, cols), BF16),
            vmem((2, n_d, n_xc, n_src * CAP, cols), BF16),
            vmem((rows, cols), F32),
            vmem((2, n_xc, n_src * CAP, cols), BF16),
            vmem((2, n_xc, n_src * CAP, cols), BF16),
            vmem((2, n_zl, n_f * n_tok, cols), F32),
            vmem((2, n_zl, n_f * n_tok, cols), BF16),
            vmem((2, n_zl, n_f * n_tok, cols), BF16),
            vmem((2, n_f, n_tok, cols), BF16),
            vmem((2, n_f, n_tok, cols), BF16),
            vmem((col_tok, slots), BF16),
            vmem((col_tok, slots), BF16),
            vmem((col_tok, slots), BF16),
            dma((3,)),
        ]
        + [dma((2, n_f)), dma((2, n_f)), dma((n_f,)), dma((n_f,))]
        + [dma((2, n_zl)), dma((2, n_zl)), dma((n_zl,)), dma((n_zl,))]
        + [dma((2, n_xc)), dma((2, n_xc))]
        + [dma((2, n_d))] * 4
        + [dma((3, n_d, 2))] * 2
        + [dma((3, n_d))] * 2
        + [dma((3, n_d, 3))] * 2
        + [dma((2, n_d))] * 2
        + [dma((2, 2))] * 2
        + [dma((2, n_xc))] * 2
        + [dma((2, n_zl))] * 2
        + [dma((2, n_f))] * 2,
        compiler_params=pltpu.CompilerParams(
            collective_id=0, has_side_effects=True, vmem_limit_bytes=60 * 1024 * 1024
        ),
    )(tokens, cotangent, routes.T, gate_fixed.T, gate_weight[0], up_weight[0], down_weight[0])
    mixed, grad_tokens, grad_down, grad_gate, grad_up = hand_over(outs)
    return mixed, grad_tokens, grad_down[None], grad_gate[None], grad_up[None]


def solution(mesh):
    n_expert, n_f, n_d = (mesh.shape[name] for name in ("expert", "fsdp", "dp"))
    n_zl = 4 if n_expert >= 16 else 2
    sizes = (n_zl, n_expert // n_zl, n_f, n_d)
    tokens = P(("expert", "fsdp", "dp"), None)
    wide = P("expert", "fsdp", "dp")
    tall = P("expert", "dp", "fsdp")
    return jax.shard_map(
        functools.partial(body, sizes),
        mesh=mesh,
        in_specs=(tokens, tokens, tokens, wide, wide, tall, tokens),
        out_specs=(tokens, tokens, tall, wide, wide),
        check_vma=False,
    )
```

```python
import functools

import jax
import jax.numpy as jnp
from jax import lax
from jax.experimental import pallas as pl
from jax.experimental.pallas import tpu as pltpu
from jax.sharding import PartitionSpec as P

F32 = jnp.float32
BF16 = jnp.bfloat16
CAP = 2


def log2(number):
    assert number & (number - 1) == 0
    return number.bit_length() - 1


def dot(a, b, ca, cb):
    return lax.dot_general(a, b, (((ca,), (cb,)), ((), ())), preferred_element_type=F32)


def kernel(
    sizes,
    tok_ref, cot_ref, routes_ref, fixed_ref, wg_hbm, wu_hbm, wd_hbm,
    mixed_ref, gtok_ref, gdown_hbm, ggate_hbm, gup_hbm,
    wg_ref, wu_ref, wd_ref, gdown, ggate, gup,
    info, xb, xs, xe, pf, rss, r1, s2, r2, av, tall_send, tall_half, tall_got, wide_send, wide_half, wide_got,
    own, isb, irb, mp, ks, kr, ls, lr, w_hi, w_lo, w_one,
    local_sem,
    sa, ra, sai, rai, sb, rb, sbi, rbi, sd, rd, se, re, sf, rf, sr, rr, sm, rm, sg, rg, sh, rh, sq, rq,
    si, ri, sk, rk, sl, rl,
):
    n_zl, n_xc, n_f, n_d = sizes
    top, n_tok = routes_ref.shape
    cols, hid = wg_ref.shape[1:]
    n_src = n_zl * n_f
    col_tok = n_src * n_tok
    slots = n_xc * n_src * CAP
    rows = slots
    part = rows // n_f

    e = lax.axis_index("expert")
    f = lax.axis_index("fsdp")
    d = lax.axis_index("dp")
    zl = e // n_xc
    xc = e % n_xc

    def at_f(j):
        return (f + j) % n_f

    def at_z(j):
        return (zl + j) % n_zl

    def at_x(j):
        return (xc + j) % n_xc

    def at_d(j):
        return (d + j + n_d) % n_d

    def device(zl_to=zl, xc_to=xc, f_to=f, d_to=d):
        return {"expert": zl_to * n_xc + xc_to, "fsdp": f_to, "dp": d_to}

    sent = []

    def copy(src, dst, send, recv, **to):
        return pltpu.make_async_remote_copy(
            src_ref=src,
            dst_ref=dst,
            send_sem=send,
            recv_sem=recv,
            device_id=device(**to),
            device_id_type=pl.DeviceIdType.MESH,
        )

    def start(one):
        one.start()
        sent.append(one)

    def start_local(source, target, number):
        one = pltpu.make_async_copy(source, target, local_sem.at[number])
        one.start()
        return one

    barrier = pltpu.get_barrier_semaphore()
    count = 0
    for limit, name, at in ((n_f, "f_to", at_f), (n_zl, "zl_to", at_z), (n_xc, "xc_to", at_x), (n_d, "d_to", at_d)):
        for j in range(1, limit):
            pl.semaphore_signal(
                barrier, inc=1, device_id=device(**{name: at(j)}), device_id_type=pl.DeviceIdType.MESH
            )
            count += 1
    weights = [
        start_local(source, target.at[0], number)
        for number, (source, target) in enumerate(((wg_hbm, wg_ref), (wu_hbm, wu_ref), (wd_hbm, wd_ref)))
    ]

    lane = lax.broadcasted_iota(jnp.int32, (n_tok, 128), 1)
    eye = lax.broadcasted_iota(jnp.int32, (n_tok, n_tok), 0) == lax.broadcasted_iota(jnp.int32, (n_tok, n_tok), 1)
    chosen_ids, fixed = routes_ref[...], fixed_ref[...]
    packed = jnp.zeros((n_tok, 128), F32)
    for number, values in enumerate((chosen_ids, lax.shift_right_logical(fixed, 8), fixed & 255)):
        values = values.astype(F32)
        for k in range(top):
            column = jnp.sum(jnp.where(eye, values[k : k + 1, :], 0.0), axis=1, keepdims=True)
            packed = jnp.where(lane == number * top + k, column, packed)
    info[zl, f] = packed.astype(BF16)
    own_cols = pl.ds(pl.multiple_of(f * cols, 128), cols)
    xb[0, zl, f] = tok_ref[:, own_cols]
    xb[1, zl, f] = cot_ref[:, own_cols]

    pl.semaphore_wait(barrier, count)

    def copy_a(a, j):
        there = at_f(j)
        src = (tok_ref, cot_ref)[a]
        columns = pl.ds(pl.multiple_of(there * cols, 128), cols)
        return copy(src.at[:, columns], xb.at[a, zl, f], sa.at[a, j], ra.at[a, j], f_to=there)

    def copy_ai(j):
        return copy(info.at[zl, f], info.at[zl, f], sai.at[j], rai.at[j], f_to=at_f(j))

    for j in range(1, n_f):
        start(copy_ai(j))
    for a in range(2):
        for j in range(1, n_f):
            start(copy_a(a, j))

    w_refs = (wg_ref, wu_ref, wd_ref)

    def half_of(rows_of, via):
        size = rows_of // 2
        return pl.ds(0, size) if via == 1 else pl.ds(size, size)

    def copy_e(s, k):
        return copy(w_refs[s].at[0], w_refs[s].at[k], se.at[s, k], re.at[s, k], d_to=at_d(k))

    def copy_far(s, k):
        piece = half_of(w_refs[s].shape[1], k)
        return copy(w_refs[s].at[k, piece], w_refs[s].at[2, piece], sf.at[s, k], rf.at[s, k], d_to=at_d(k))

    def pass_weights(s):
        for k in (1, n_d - 1):
            copy_e(s, k).wait_recv()
            start(copy_far(s, k))

    def take_far(s):
        for k in (1, n_d - 1):
            copy_far(s, k).wait_recv()

    for s in range(3):
        weights[s].wait()
        for k in (1, n_d - 1):
            start(copy_e(s, k))

    def copy_b(a, j):
        return copy(xb.at[a, zl], xb.at[a, zl], sb.at[a, j], rb.at[a, j], zl_to=at_z(j))

    def copy_bi(j):
        return copy(info.at[zl], info.at[zl], sbi.at[j], rbi.at[j], zl_to=at_z(j))

    for j in range(1, n_f):
        copy_ai(j).wait_recv()
    for j in range(1, n_zl):
        start(copy_bi(j))
    for a in range(2):
        for j in range(1, n_f):
            copy_a(a, j).wait_recv()
        for j in range(1, n_zl):
            start(copy_b(a, j))

    for j in range(1, n_zl):
        copy_bi(j).wait_recv()
    table = info[...].reshape(col_tok, 128).astype(F32)
    slot = lax.broadcasted_iota(jnp.int32, (col_tok, slots), 1)
    token = lax.broadcasted_iota(jnp.int32, (col_tok, slots), 0)
    slot_expert = (zl * n_xc + lax.shift_right_logical(slot, log2(n_src * CAP))).astype(F32)
    slot_source = lax.shift_right_logical(slot, log2(CAP)) & (n_src - 1)
    slot_rank = (slot & (CAP - 1)).astype(F32)
    hit = [table[:, k : k + 1] == slot_expert for k in range(top)]
    named = functools.reduce(jnp.logical_or, hit)
    before_row = lax.broadcasted_iota(jnp.int32, (col_tok, col_tok), 0)
    before_col = lax.broadcasted_iota(jnp.int32, (col_tok, col_tok), 1)
    shift = log2(n_tok)
    earlier = (before_col < before_row) & (
        lax.shift_right_logical(before_col, shift) == lax.shift_right_logical(before_row, shift)
    )
    rank = dot(jnp.where(earlier, 1.0, 0.0).astype(BF16), jnp.where(named, 1.0, 0.0).astype(BF16), 1, 0)
    chosen = named & (rank == slot_rank) & (lax.shift_right_logical(token, shift) == slot_source)
    weight = jnp.zeros((col_tok, slots), F32)
    for k in range(top):
        value = table[:, top + k : top + k + 1] * 256.0 + table[:, 2 * top + k : 2 * top + k + 1]
        weight = jnp.where(hit[k], value * (1.0 / 65536.0), weight)
    weight = jnp.where(chosen, weight, 0.0)
    high = weight.astype(BF16)
    w_hi[...] = high
    w_lo[...] = (weight - high.astype(F32)).astype(BF16)
    w_one[...] = jnp.where(chosen, 1.0, 0.0).astype(BF16)

    def copy_d(a, j):
        there = at_x(j)
        return copy(xs.at[a, there], xe.at[a, xc], sd.at[a, j], rd.at[a, j], xc_to=there)

    def send_d(a):
        for j in range(1, n_zl):
            copy_b(a, j).wait_recv()
        table_rows = xb[a].reshape(col_tok, cols)
        if a == 0:
            picked = dot(w_one[...], table_rows, 0, 0)
        else:
            picked = dot(w_hi[...], table_rows, 0, 0) + dot(w_lo[...], table_rows, 0, 0)
        xs[a] = picked.astype(BF16).reshape(n_xc, n_src * CAP, cols)
        xe[a, xc] = xs[a, xc]
        for j in range(1, n_xc):
            start(copy_d(a, j))

    def take_d(a):
        for j in range(1, n_xc):
            copy_d(a, j).wait_recv()

    def sides(turn):
        step = 1 - 2 * ((f + turn) % 2)
        return (f + step + n_f) % n_f, (f - step + n_f) % n_f

    def sides_r(s, k):
        return sides(s if s < 2 else k % 2)

    def copy_r(s, k, which):
        first, _ = sides_r(s, k)
        quarter = at_f(2) if which == 0 else first
        return copy(
            rss.at[s, k, quarter], r1.at[s, k, quarter], sr.at[s, k, which], rr.at[s, k, which], f_to=first
        )

    def copy_m(s, k):
        _, second = sides_r(s, k)
        return copy(s2.at[s, k], r2.at[s, k], sm.at[s, k], rm.at[s, k], f_to=second)

    def part_of(quarter):
        return pl.ds(pl.multiple_of(quarter * part, part), part)

    def scatter(s, k):
        operand = xe[0 if s < 2 else 1].reshape(rows, cols)
        product = dot(operand, w_refs[s][k], 1, 0 if s < 2 else 1)
        pf[s, k] = product
        rss[s, k] = product.astype(BF16).reshape(n_f, part, hid)
        for which in range(2):
            start(copy_r(s, k, which))

    def scatter_more(s, k):
        copy_r(s, k, 0).wait_recv()
        _, second = sides_r(s, k)
        s2[s, k] = (pf[s, k, part_of(second), :] + r1[s, k, second].astype(F32)).astype(BF16)
        start(copy_m(s, k))

    def total_of(s, k):
        copy_r(s, k, 1).wait_recv()
        copy_m(s, k).wait_recv()
        return pf[s, k, part_of(f), :] + r1[s, k, f].astype(F32) + r2[s, k].astype(F32)

    def copy_g(s, k, which):
        first, second = sides(k % 2 if s == 0 else s - 1)
        mine = av.at[s, k, second if which == 2 else f]
        return copy(mine, mine, sg.at[s, k, which], rg.at[s, k, which], f_to=second if which == 0 else first)

    def activations(k):
        gate = pf[0, k, part_of(f), :]
        sigmoid = jax.nn.sigmoid(gate)
        return gate, pf[1, k, part_of(f), :], sigmoid, gate * sigmoid

    def gather_hidden(k):
        for s in range(2):
            pf[s, k, part_of(f), :] = total_of(s, k)
        _, up, _, swish = activations(k)
        av[0, k, f] = (swish * up).astype(BF16)
        for which in range(2):
            start(copy_g(0, k, which))

    def gather_grads(k):
        grad = total_of(2, k)
        gate, up, sigmoid, swish = activations(k)
        av[1, k, f] = (grad * up * sigmoid * (1.0 + gate * (1.0 - sigmoid))).astype(BF16)
        av[2, k, f] = (grad * swish).astype(BF16)
        for which in range(2):
            for s in (1, 2):
                start(copy_g(s, k, which))

    def gather_more(a, k):
        for s in (0,) if a == 0 else (1, 2):
            copy_g(s, k, 0).wait_recv()
            start(copy_g(s, k, 2))

    def gathered(a, k):
        for s in (0,) if a == 0 else (1, 2):
            for which in (1, 2):
                copy_g(s, k, which).wait_recv()

    def rows_of(s, k):
        return av[s, k].reshape(rows, hid)

    def output(a, k, first=False):
        gathered(a, k)
        if a == 0:
            product = dot(rows_of(0, k), wd_ref[k], 1, 0)
        else:
            product = dot(rows_of(1, k), wg_ref[k], 1, 1) + dot(rows_of(2, k), wu_ref[k], 1, 1)
        own[a] = product if first else own[a] + product

    grads = (gdown, ggate, gup)

    def buffers_of(s):
        if s == 0:
            return tall_send, tall_half, tall_got
        return wide_send.at[s - 1], wide_half.at[s - 1], wide_got.at[s - 1]

    def weight_grad(s, k):
        if s == 0:
            return dot(rows_of(0, k), xe[1].reshape(rows, cols), 0, 0)
        return dot(xe[0].reshape(rows, cols), rows_of(s, k), 0, 0)

    def copy_half(s, via):
        source, target, _ = buffers_of(s)
        piece = half_of(grads[s].shape[0], via)
        number = 0 if via == 1 else 1
        return copy(source.at[2, piece], target.at[piece], sq.at[s, number], rq.at[s, number], d_to=at_d(via))

    def copy_h(s, k):
        source, _, target = buffers_of(s)
        return copy(source.at[k], target.at[k], sh.at[s, k], rh.at[s, k], d_to=at_d(-k))

    def send_far(s):
        source, _, _ = buffers_of(s)
        source[2] = weight_grad(s, 2).astype(BF16)
        for via in (1, n_d - 1):
            start(copy_half(s, via))

    def send_near(s, k):
        source, joined, _ = buffers_of(s)
        via = n_d - k
        term = weight_grad(s, k)
        size = term.shape[0] // 2
        copy_half(s, via).wait_recv()
        if via == 1:
            source[k, :size] = (term[:size] + joined[:size].astype(F32)).astype(BF16)
            source[k, size:] = term[size:].astype(BF16)
        else:
            source[k, :size] = term[:size].astype(BF16)
            source[k, size:] = (term[size:] + joined[size:].astype(F32)).astype(BF16)
        start(copy_h(s, k))

    def keep(s):
        _, _, got = buffers_of(s)
        term = weight_grad(s, 0)
        for k in (1, n_d - 1):
            copy_h(s, k).wait_recv()
        grads[s][...] = term + got[1].astype(F32) + got[n_d - 1].astype(F32)
        return start_local(grads[s], (gdown_hbm, ggate_hbm, gup_hbm)[s], s)

    def copy_i(a, j):
        there = at_x(j)
        return copy(isb.at[a, there], irb.at[a, xc], si.at[a, j], ri.at[a, j], xc_to=there)

    def send_i(a):
        isb[a] = own[a].astype(BF16).reshape(n_xc, n_src * CAP, cols)
        irb[a, xc] = isb[a, xc]
        for j in range(1, n_xc):
            start(copy_i(a, j))

    def copy_k(a, j):
        there = at_z(j)
        return copy(ks.at[a, there], kr.at[a, zl], sk.at[a, j], rk.at[a, j], zl_to=there)

    def send_k(a):
        for j in range(1, n_xc):
            copy_i(a, j).wait_recv()
        returned = irb[a].reshape(slots, cols)
        if a == 0:
            value = dot(w_hi[...], returned, 1, 0) + dot(w_lo[...], returned, 1, 0)
        else:
            value = dot(w_one[...], returned, 1, 0)
        value = value.reshape(n_zl, n_f * n_tok, cols)
        mp[a] = value
        ks[a] = value.astype(BF16)
        for j in range(1, n_zl):
            start(copy_k(a, j))

    def copy_l(a, j):
        there = at_f(j)
        return copy(ls.at[a, there], lr.at[a, f], sl.at[a, j], rl.at[a, j], f_to=there)

    def send_l(a):
        for j in range(1, n_zl):
            copy_k(a, j).wait_recv()
        total = mp[a, zl]
        for j in range(1, n_zl):
            total = total + kr[a, at_z(j)].astype(F32)
        ls[a] = total.astype(BF16).reshape(n_f, n_tok, cols)
        lr[a, f] = ls[a, f]
        for j in range(1, n_f):
            start(copy_l(a, j))

    def finish(a):
        for j in range(1, n_f):
            copy_l(a, j).wait_recv()
        for owner in range(n_f):
            (mixed_ref, gtok_ref)[a][:, owner * cols : (owner + 1) * cols] = lr[a, owner]

    send_d(0)
    pass_weights(0)
    take_d(0)
    scatter(0, 0)
    scatter(1, 0)
    scatter(0, 1)
    pass_weights(1)
    scatter(1, 1)
    send_d(1)
    scatter(0, 3)
    scatter(1, 3)
    scatter_more(0, 0)
    scatter_more(1, 0)
    take_d(1)
    scatter(2, 0)
    pass_weights(2)
    scatter(2, 1)
    scatter_more(0, 1)
    scatter_more(1, 1)
    scatter(2, 3)
    take_far(0)
    scatter(0, 2)
    scatter_more(0, 3)
    scatter_more(1, 3)
    take_far(1)
    scatter(1, 2)
    scatter_more(2, 0)
    take_far(2)
    scatter(2, 2)
    scatter_more(2, 1)
    gather_hidden(0)
    scatter_more(2, 3)
    gather_hidden(1)
    for s in range(3):
        scatter_more(s, 2)
    gather_hidden(3)
    gather_more(0, 0)
    gather_hidden(2)
    gather_more(0, 1)
    gather_grads(2)
    gather_more(0, 3)
    output(0, 0, True)
    output(0, 1)
    gather_grads(1)
    gather_more(0, 2)
    output(0, 3)
    gather_grads(3)
    gather_more(1, 2)
    output(0, 2)
    send_i(0)
    send_far(0)
    gather_grads(0)
    gather_more(1, 1)
    output(1, 2, True)
    send_far(1)
    send_far(2)
    send_near(0, 1)
    send_near(0, 3)
    gather_more(1, 3)
    output(1, 1)
    send_near(1, 1)
    send_near(2, 1)
    gather_more(1, 0)
    send_k(0)
    output(1, 3)
    send_near(1, 3)
    send_near(2, 3)
    output(1, 0)
    send_i(1)
    results = [keep(0)]
    send_k(1)
    send_l(0)
    results.append(keep(1))
    send_l(1)
    results.append(keep(2))
    finish(0)
    finish(1)
    for one in sent:
        one.wait_send()
    for one in results:
        one.wait()


def hand_over_kernel(*refs):
    count = (len(refs) - 1) // 3
    sources, targets, held, sem = refs[:count], refs[count : 2 * count], refs[2 * count : 3 * count], refs[-1]
    into = [pltpu.make_async_copy(sources[i], held[i], sem.at[0, i]) for i in range(count)]
    out = [pltpu.make_async_copy(held[i], targets[i], sem.at[1, i]) for i in range(count)]
    for one in into:
        one.start()
    for i in range(count):
        into[i].wait()
        out[i].start()
    for one in out:
        one.wait()


def hand_over(arrays):
    anywhere = pl.BlockSpec(memory_space=pl.ANY)
    return pl.pallas_call(
        hand_over_kernel,
        out_shape=tuple(jax.ShapeDtypeStruct(one.shape, one.dtype) for one in arrays),
        in_specs=[anywhere] * len(arrays),
        out_specs=[anywhere] * len(arrays),
        scratch_shapes=[pltpu.VMEM(one.shape, one.dtype) for one in arrays]
        + [pltpu.SemaphoreType.DMA((2, len(arrays)))],
    )(*arrays)


def body(sizes, tokens, routes, gate_fixed, gate_weight, up_weight, down_weight, cotangent):
    n_zl, n_xc, n_f, n_d = sizes
    n_tok, width = tokens.shape
    cols, hid = gate_weight.shape[1:]
    n_src = n_zl * n_f
    col_tok = n_src * n_tok
    slots = n_xc * n_src * CAP
    rows = slots
    part = rows // n_f
    vmem = pltpu.VMEM
    dma = pltpu.SemaphoreType.DMA
    outs = pl.pallas_call(
        functools.partial(kernel, sizes),
        out_shape=(
            jax.ShapeDtypeStruct((n_tok, width), BF16),
            jax.ShapeDtypeStruct((n_tok, width), BF16),
            jax.ShapeDtypeStruct((hid, cols), F32),
            jax.ShapeDtypeStruct((cols, hid), F32),
            jax.ShapeDtypeStruct((cols, hid), F32),
        ),
        in_specs=[pl.BlockSpec(memory_space=pltpu.VMEM)] * 4 + [pl.BlockSpec(memory_space=pl.ANY)] * 3,
        out_specs=[pl.BlockSpec(memory_space=pltpu.VMEM)] * 2 + [pl.BlockSpec(memory_space=pl.ANY)] * 3,
        scratch_shapes=[
            vmem((n_d, cols, hid), BF16),
            vmem((n_d, cols, hid), BF16),
            vmem((n_d, hid, cols), BF16),
            vmem((hid, cols), F32),
            vmem((cols, hid), F32),
            vmem((cols, hid), F32),
            vmem((n_zl, n_f, n_tok, 128), BF16),
            vmem((2, n_zl, n_f, n_tok, cols), BF16),
            vmem((2, n_xc, n_src * CAP, cols), BF16),
            vmem((2, n_xc, n_src * CAP, cols), BF16),
            vmem((3, n_d, rows, hid), F32),
            vmem((3, n_d, n_f, part, hid), BF16),
            vmem((3, n_d, n_f, part, hid), BF16),
            vmem((3, n_d, part, hid), BF16),
            vmem((3, n_d, part, hid), BF16),
            vmem((3, n_d, n_f, part, hid), BF16),
            vmem((n_d, hid, cols), BF16),
            vmem((hid, cols), BF16),
            vmem((n_d, hid, cols), BF16),
            vmem((2, n_d, cols, hid), BF16),
            vmem((2, cols, hid), BF16),
            vmem((2, n_d, cols, hid), BF16),
            vmem((2, rows, cols), F32),
            vmem((2, n_xc, n_src * CAP, cols), BF16),
            vmem((2, n_xc, n_src * CAP, cols), BF16),
            vmem((2, n_zl, n_f * n_tok, cols), F32),
            vmem((2, n_zl, n_f * n_tok, cols), BF16),
            vmem((2, n_zl, n_f * n_tok, cols), BF16),
            vmem((2, n_f, n_tok, cols), BF16),
            vmem((2, n_f, n_tok, cols), BF16),
            vmem((col_tok, slots), BF16),
            vmem((col_tok, slots), BF16),
            vmem((col_tok, slots), BF16),
            dma((3,)),
        ]
        + [dma((2, n_f)), dma((2, n_f)), dma((n_f,)), dma((n_f,))]
        + [dma((2, n_zl)), dma((2, n_zl)), dma((n_zl,)), dma((n_zl,))]
        + [dma((2, n_xc)), dma((2, n_xc))]
        + [dma((3, n_d))] * 4
        + [dma((3, n_d, 2))] * 2
        + [dma((3, n_d))] * 2
        + [dma((3, n_d, 3))] * 2
        + [dma((3, n_d))] * 2
        + [dma((3, 2))] * 2
        + [dma((2, n_xc))] * 2
        + [dma((2, n_zl))] * 2
        + [dma((2, n_f))] * 2,
        compiler_params=pltpu.CompilerParams(
            collective_id=0, has_side_effects=True, vmem_limit_bytes=60 * 1024 * 1024
        ),
    )(tokens, cotangent, routes.T, gate_fixed.T, gate_weight[0], up_weight[0], down_weight[0])
    mixed, grad_tokens, grad_down, grad_gate, grad_up = hand_over(outs)
    return mixed, grad_tokens, grad_down[None], grad_gate[None], grad_up[None]


def solution(mesh):
    n_expert, n_f, n_d = (mesh.shape[name] for name in ("expert", "fsdp", "dp"))
    n_zl = 4 if n_expert >= 16 else 2
    sizes = (n_zl, n_expert // n_zl, n_f, n_d)
    tokens = P(("expert", "fsdp", "dp"), None)
    wide = P("expert", "fsdp", "dp")
    tall = P("expert", "dp", "fsdp")
    return jax.shard_map(
        functools.partial(body, sizes),
        mesh=mesh,
        in_specs=(tokens, tokens, tokens, wide, wide, tall, tokens),
        out_specs=(tokens, tokens, tall, wide, wide),
        check_vma=False,
    )
```
